32 devices in a mesh: dp: 2 (over z, core), sp: 16 (over x, y).
Axes of the slice: x: 4, y: 4, z: 1, core: 2. Of those that a mesh axis runs over, the one named last changes fastest.
The devices are a block of a 4x4x8 slice.
Arguments:
- q: bfloat16 [64, 8, 256], P('dp'), parts along dimension 0
- k: bfloat16 [64, 8192, 8, 256], P('dp', 'sp'), parts along dimension 0
- v: bfloat16 [64, 8192, 8, 256], P('dp', 'sp'), parts along dimension 0
Outputs:
- q: bfloat16 [64, 8, 256], P('dp'), parts along dimension 0
There are 2 independent parts. The reference program is written for one: setup_inputs(seed, part) draws one part's arguments, and reference() takes and returns one part's arrays. A program takes and returns all parts, laid end to end along the dimension named above; each array names one.
All inputs are finite; a program needn't handle non-finite values.
Results may differ from the reference program's by a relative error of at most 0.012.
Values are sent between devices in bfloat16 or wider.
A program may use at most 768 MiB of HBM per device.

```python
import jax
import jax.numpy as jnp

BATCH = 32
CACHE = 8192
HEADS = 8
KV_HEADS = 8
HEAD = 256


def setup_inputs(seed: int = 0, part: int = 0) -> dict:
    kq, kk, kv = (jax.random.fold_in(k, part) for k in jax.random.split(jax.random.key(seed), 3))
    return {
        "q": (3 * jax.random.normal(kq, (BATCH, HEADS, HEAD), jnp.float32)).astype(jnp.bfloat16),
        "k": jax.random.normal(kk, (BATCH, CACHE, KV_HEADS, HEAD), jnp.float32).astype(jnp.bfloat16),
        "v": jax.random.normal(kv, (BATCH, CACHE, KV_HEADS, HEAD), jnp.float32).astype(jnp.bfloat16),
    }


def einsum(form, a, b):
    return jnp.einsum(form, a.astype(jnp.float32), b.astype(jnp.float32))


def reference(q, k, v):
    grouped = q.reshape(BATCH, KV_HEADS, -1, HEAD)
    scores = einsum("bgsd,bugd->bgsu", grouped, k) * HEAD**-0.5
    weights = jax.nn.softmax(scores, -1).astype(jnp.bfloat16)
    return einsum("bgsu,bugd->bgsd", weights, v).astype(jnp.bfloat16).reshape(BATCH, HEADS, HEAD)
```

```python
import functools
import math

import jax
import jax.numpy as jnp
from jax import lax
from jax.experimental import pallas as pl
from jax.experimental.pallas import tpu as pltpu
from jax.sharding import PartitionSpec as P

SLOTS = 6
CHUNKS = (2, 1, 1)
LANES = 128
AXIS = "sp"
MESH = pl.DeviceIdType.MESH
COLLECTIVE = 0


def offsets(n):
    side = math.isqrt(n)
    near = lambda a: min(a, side - a)
    return sorted(range(1, n), key=lambda o: -(near(o // side % side) + near(o % side)))


def kernel(
    n, seqs, rows, heads, width, scale,
    q_hbm, k_hbm, v_hbm, o_hbm,
    qbuf, kbuf, vbuf, w0, w1, part, stat, out,
    rs_data, rs_stat, dr_data, dr_stat,
    qsem, ksem, vsem, osem,
    rs_send, rs_recv, ag_send, ag_recv, dr_send, dr_recv,
):
    me = lax.axis_index(AXIS)
    direct = sum(CHUNKS)
    ringed = seqs - direct
    starts = [ringed + sum(CHUNKS[:c]) for c in range(len(CHUNKS))]
    order = offsets(n)

    def k_copy(i):
        slot = lax.rem(i, SLOTS)
        return pltpu.make_async_copy(k_hbm.at[i], kbuf.at[slot], ksem.at[slot])

    def v_copy(i):
        slot = lax.rem(i, SLOTS)
        return pltpu.make_async_copy(v_hbm.at[i], vbuf.at[slot], vsem.at[slot])

    q_copy = pltpu.make_async_copy(q_hbm, qbuf, qsem)
    q_copy.start()
    k_copy(0).start()
    for i in range(SLOTS - 1):
        k_copy(i + 1).start()
        v_copy(i).start()

    barrier = pltpu.get_barrier_semaphore()
    for o in order:
        pl.semaphore_signal(barrier, inc=1, device_id={AXIS: lax.rem(me + o, n)}, device_id_type=MESH)
    pl.semaphore_wait(barrier, n - 1)

    lane = lax.broadcasted_iota(jnp.int32, (heads, LANES), 1)
    sub = lax.broadcasted_iota(jnp.int32, (heads, LANES), 0)
    own = lane % heads == sub
    diag = lane == sub
    diag2 = lane == sub + heads

    def look(i, w_ref):
        slot = lax.rem(i, SLOTS)
        s = lax.dot_general(qbuf[i], kbuf[slot], (((1,), (1,)), ((), ())), preferred_element_type=jnp.float32)
        cols = [jnp.where(own, s[:, c : c + LANES], -jnp.inf) for c in range(0, rows, LANES)]
        high = functools.reduce(jnp.maximum, cols)
        high = jnp.max(high, 1, keepdims=True)
        total = jnp.zeros((heads, LANES), jnp.float32)
        for c, col in enumerate(cols):
            w = jnp.exp((col - high) * scale)
            total = total + w
            w_ref[:, c * LANES : (c + 1) * LANES] = w.astype(jnp.bfloat16)
        total = jnp.sum(total, 1, keepdims=True)
        row = jnp.where(diag, high * scale, 0.0) + jnp.where(diag2, total, 0.0)
        stat[i] = jnp.sum(row, 0, keepdims=True)

    def see(i, w_ref):
        slot = lax.rem(i, SLOTS)
        o = jnp.dot(w_ref[...], vbuf[slot], preferred_element_type=jnp.float32)
        part[i] = o.astype(jnp.bfloat16)

    def together(data, stats):
        high = functools.reduce(jnp.maximum, stats)
        f = [jnp.exp(s - high) for s in stats]
        total = functools.reduce(jnp.add, [a * pltpu.roll(s, LANES - heads, 1) for a, s in zip(f, stats)])
        column = lambda r: jnp.sum(jnp.where(diag, jnp.broadcast_to(r, (heads, LANES)), 0.0), 1, keepdims=True)
        seen = functools.reduce(jnp.add, [column(a) * d.astype(jnp.float32) for a, d in zip(f, data)])
        return (seen / column(total)).astype(jnp.bfloat16)

    def rs_copies(i):
        b, owner = i // n, lax.rem(i, n)
        return [
            pltpu.make_async_remote_copy(
                src_ref=src.at[i], dst_ref=dst.at[b, me], send_sem=rs_send.at[x, i], recv_sem=rs_recv.at[x, b, me],
                device_id={AXIS: owner}, device_id_type=MESH,
            )
            for x, (src, dst) in enumerate(((part, rs_data), (stat, rs_stat)))
        ]

    def rs_start(i):
        b, owner = i // n, lax.rem(i, n)

        @pl.when(owner != me)
        def _():
            for c in rs_copies(i):
                c.start()

        @pl.when(owner == me)
        def _():
            rs_data[b, me] = part[i]
            rs_stat[b, me] = stat[i]

    def ag_copy(b, o):
        s, peer = b * n + me, lax.rem(me + o, n)
        return pltpu.make_async_remote_copy(
            src_ref=out.at[s], dst_ref=out.at[s], send_sem=ag_send.at[b, o], recv_sem=ag_recv.at[s],
            device_id={AXIS: peer}, device_id_type=MESH,
        )

    def ag_start(b):
        @pl.when(b * n + me < ringed)
        def _():
            for o in order:
                peer = lax.rem(me + o, n)
                for x, ref in enumerate((rs_data, rs_stat)):
                    pltpu.make_async_remote_copy(
                        src_ref=ref.at[b, peer], dst_ref=ref.at[b, peer], send_sem=rs_send.at[x, 0], recv_sem=rs_recv.at[x, b, peer],
                        device_id={AXIS: peer}, device_id_type=MESH,
                    ).wait_recv()
            out[b * n + me] = together([rs_data[b, d] for d in range(n)], [rs_stat[b, d] for d in range(n)])
            for o in order:
                ag_copy(b, o).start()

    def dr_copies(c, o, peer_slot):
        at, count = starts[c], CHUNKS[c]
        return [
            pltpu.make_async_remote_copy(
                src_ref=src.at[pl.ds(at, count)], dst_ref=dst.at[peer_slot, pl.ds(at - ringed, count)],
                send_sem=dr_send.at[x, c, o], recv_sem=dr_recv.at[x, c, peer_slot],
                device_id={AXIS: lax.rem(me + o, n)}, device_id_type=MESH,
            )
            for x, (src, dst) in enumerate(((part, dr_data), (stat, dr_stat)))
        ]

    def dr_start(c):
        for o in order:
            for copy in dr_copies(c, o, me):
                copy.start()
        for t in range(CHUNKS[c]):
            dr_data[me, starts[c] - ringed + t] = part[starts[c] + t]
            dr_stat[me, starts[c] - ringed + t] = stat[starts[c] + t]

    def dr_end(c):
        for o in order:
            for copy in dr_copies(c, n - o, lax.rem(me + o, n)):
                copy.wait_recv()
        for t in range(CHUNKS[c]):
            at = starts[c] - ringed + t
            out[starts[c] + t] = together([dr_data[d, at] for d in range(n)], [dr_stat[d, at] for d in range(n)])

    q_copy.wait()
    k_copy(0).wait()
    look(0, w0)

    def body(i, w_now, w_next):
        k_copy(i + 1).wait()
        v_copy(i).wait()
        look(i + 1, w_next)
        see(i, w_now)

    batches = -(-ringed // n)
    ag_at = [min((b + 1) * n, ringed) // 2 + 2 for b in range(batches)]

    @pl.loop(0, seqs // 2 - 1)
    def _(p):
        i = 2 * p

        @pl.when(i + SLOTS < seqs)
        def _():
            k_copy(i + SLOTS).start()

        @pl.when(i - 1 + SLOTS < seqs)
        def _():
            v_copy(i - 1 + SLOTS).start()

        body(i, w0, w1)

        @pl.when((i > 0) & (i - 1 < ringed))
        def _():
            rs_start(i - 1)

        @pl.when(i + 1 + SLOTS < seqs)
        def _():
            k_copy(i + 1 + SLOTS).start()

        @pl.when(i + SLOTS < seqs)
        def _():
            v_copy(i + SLOTS).start()

        body(i + 1, w1, w0)

        @pl.when(i < ringed)
        def _():
            rs_start(i)

        for b in range(batches):
            if ag_at[b] < seqs // 2 - 1:

                @pl.when(p == ag_at[b])
                def _():
                    ag_start(b)

    if ringed == seqs - 2:
        rs_start(ringed - 1)
    for c in range(len(CHUNKS)):
        if starts[c] + CHUNKS[c] <= seqs - 2:
            dr_start(c)
    body(seqs - 2, w0, w1)
    for c in range(len(CHUNKS)):
        if starts[c] + CHUNKS[c] == seqs - 1:
            dr_start(c)
    for b in range(batches):
        if ag_at[b] >= seqs // 2 - 1:
            ag_start(b)
    v_copy(seqs - 1).wait()
    see(seqs - 1, w1)
    dr_start(len(CHUNKS) - 1)

    @pl.loop(0, ringed)
    def _(s):
        b, owner = s // n, lax.rem(s, n)

        @pl.when(owner != me)
        def _():
            pltpu.make_async_remote_copy(
                src_ref=out.at[s], dst_ref=out.at[s], send_sem=ag_send.at[b, 0], recv_sem=ag_recv.at[s],
                device_id={AXIS: owner}, device_id_type=MESH,
            ).wait_recv()
            for c in rs_copies(s):
                c.wait_send()

    first = pltpu.make_async_copy(out.at[pl.ds(0, ringed)], o_hbm.at[pl.ds(0, ringed)], osem.at[0])
    first.start()
    for c in range(len(CHUNKS)):
        dr_end(c)
    last = pltpu.make_async_copy(out.at[pl.ds(ringed, direct)], o_hbm.at[pl.ds(ringed, direct)], osem.at[1])
    last.start()
    for b in range(batches):

        @pl.when(b * n + me < ringed)
        def _():
            for o in order:
                ag_copy(b, o).wait_send()

    for c in range(len(CHUNKS)):
        for o in order:
            for copy in dr_copies(c, o, me):
                copy.wait_send()
    first.wait()
    last.wait()


def solution(mesh):
    n = mesh.shape[AXIS]

    def step(q, k, v):
        seqs, tokens, heads, width = k.shape
        rows, direct = tokens * heads, sum(CHUNKS)
        ringed = seqs - direct
        batches, chunks = -(-ringed // n), len(CHUNKS)
        flat = lambda a: a.reshape(seqs, rows, width)
        hbm = pl.BlockSpec(memory_space=pl.ANY)
        dma = pltpu.SemaphoreType.DMA
        return pl.pallas_call(
            functools.partial(kernel, n, seqs, rows, heads, width, width**-0.5),
            out_shape=jax.ShapeDtypeStruct(q.shape, q.dtype),
            in_specs=[hbm] * 3,
            out_specs=hbm,
            scratch_shapes=[
                pltpu.VMEM(q.shape, q.dtype),
                pltpu.VMEM((SLOTS, rows, width), k.dtype),
                pltpu.VMEM((SLOTS, rows, width), v.dtype),
                pltpu.VMEM((heads, rows), jnp.bfloat16),
                pltpu.VMEM((heads, rows), jnp.bfloat16),
                pltpu.VMEM((seqs, heads, width), jnp.bfloat16),
                pltpu.VMEM((seqs, 1, LANES), jnp.float32),
                pltpu.VMEM((seqs, heads, width), jnp.bfloat16),
                pltpu.VMEM((batches, n, heads, width), jnp.bfloat16),
                pltpu.VMEM((batches, n, 1, LANES), jnp.float32),
                pltpu.VMEM((n, direct, heads, width), jnp.bfloat16),
                pltpu.VMEM((n, direct, 1, LANES), jnp.float32),
                dma(()),
                dma((SLOTS,)),
                dma((SLOTS,)),
                dma((2,)),
                dma((2, ringed)),
                dma((2, batches, n)),
                dma((batches, n)),
                dma((ringed,)),
                dma((2, chunks, n)),
                dma((2, chunks, n)),
            ],
            compiler_params=pltpu.CompilerParams(
                collective_id=COLLECTIVE, has_side_effects=True, vmem_limit_bytes=60 * 1024 * 1024
            ),
            cost_estimate=pl.CostEstimate(flops=4 * seqs * rows * width, bytes_accessed=2 * k.size * 2, transcendentals=0),
            name="attend",
        )(q, flat(k), flat(v))

    return jax.shard_map(
        step,
        mesh=mesh,
        in_specs=(P("dp", None, None), P("dp", AXIS, None, None), P("dp", AXIS, None, None)),
        out_specs=P("dp", None, None),
        check_vma=False,
    )
```

```python
import functools
import math

import jax
import jax.numpy as jnp
from jax import lax
from jax.experimental import pallas as pl
from jax.experimental.pallas import tpu as pltpu
from jax.sharding import PartitionSpec as P

SLOTS = 4
EARLY = 5
TAIL = 4
CHUNKS = (2, 1, 1)
LANES = 128
AXIS = "sp"
MESH = pl.DeviceIdType.MESH
COLLECTIVE = 0


def offsets(n):
    side = math.isqrt(n)
    near = lambda a: min(a, side - a)
    return sorted(range(1, n), key=lambda o: -(near(o // side % side) + near(o % side)))


def kernel(
    n, seqs, rows, heads, width, scale,
    q_hbm, k_hbm, v_hbm, out,
    qbuf, kbuf, vbuf, w0, w1, part, stat,
    rs_data, rs_stat, dr_data, dr_stat,
    qsem, ksem, vsem, tsem,
    rs_send, rs_recv, ag_send, ag_recv, dr_send, dr_recv,
):
    me = lax.axis_index(AXIS)
    direct = sum(CHUNKS)
    ringed = seqs - direct
    starts = [ringed + sum(CHUNKS[:c]) for c in range(len(CHUNKS))]
    order = offsets(n)

    def k_copy(i):
        slot = lax.rem(i, SLOTS)
        return pltpu.make_async_copy(k_hbm.at[i], kbuf.at[slot], ksem.at[slot])

    def v_copy(i):
        slot = lax.rem(i, SLOTS)
        return pltpu.make_async_copy(v_hbm.at[i], vbuf.at[slot], vsem.at[slot])

    def v_piece(t):
        at, slot = pl.ds(t * (rows // TAIL), rows // TAIL), (seqs - 1) % SLOTS
        return pltpu.make_async_copy(v_hbm.at[seqs - 1, at], vbuf.at[slot, at], tsem.at[t])

    def v_start(i):
        @pl.when(i < seqs - 1)
        def _():
            v_copy(i).start()

        @pl.when(i == seqs - 1)
        def _():
            for t in range(TAIL):
                v_piece(t).start()

    q_copy = pltpu.make_async_copy(q_hbm, qbuf, qsem)
    q_copy.start()
    k_copy(0).start()
    for i in range(SLOTS - 1):
        k_copy(i + 1).start()
        v_copy(i).start()

    barrier = pltpu.get_barrier_semaphore()
    for o in order:
        pl.semaphore_signal(barrier, inc=1, device_id={AXIS: lax.rem(me + o, n)}, device_id_type=MESH)

    lane = lax.broadcasted_iota(jnp.int32, (heads, LANES), 1)
    sub = lax.broadcasted_iota(jnp.int32, (heads, LANES), 0)
    own = lane % heads == sub
    diag = lane == sub
    diag2 = lane == sub + heads

    def look(i, w_ref):
        slot = lax.rem(i, SLOTS)
        s = lax.dot_general(qbuf[i], kbuf[slot], (((1,), (1,)), ((), ())), preferred_element_type=jnp.float32)
        cols = [jnp.where(own, s[:, c : c + LANES], -jnp.inf) for c in range(0, rows, LANES)]
        high = functools.reduce(jnp.maximum, cols)
        high = jnp.max(high, 1, keepdims=True)
        total = jnp.zeros((heads, LANES), jnp.float32)
        for c, col in enumerate(cols):
            w = jnp.exp((col - high) * scale)
            total = total + w
            w_ref[:, c * LANES : (c + 1) * LANES] = w.astype(jnp.bfloat16)
        total = jnp.sum(total, 1, keepdims=True)
        row = jnp.where(diag, high * scale, 0.0) + jnp.where(diag2, total, 0.0)
        stat[i] = jnp.sum(row, 0, keepdims=True)

    def see(i, w_ref):
        slot = lax.rem(i, SLOTS)
        o = jnp.dot(w_ref[...], vbuf[slot], preferred_element_type=jnp.float32)
        part[i] = o.astype(jnp.bfloat16)

    def together(data, stats):
        high = functools.reduce(jnp.maximum, stats)
        f = [jnp.exp(s - high) for s in stats]
        total = functools.reduce(jnp.add, [a * pltpu.roll(s, LANES - heads, 1) for a, s in zip(f, stats)])
        column = lambda r: jnp.sum(jnp.where(diag, jnp.broadcast_to(r, (heads, LANES)), 0.0), 1, keepdims=True)
        seen = functools.reduce(jnp.add, [column(a) * d.astype(jnp.float32) for a, d in zip(f, data)])
        return (seen / column(total)).astype(jnp.bfloat16)

    def send(src, dst, send_sem, recv_sem, peer):
        return pltpu.make_async_remote_copy(
            src_ref=src, dst_ref=dst, send_sem=send_sem, recv_sem=recv_sem, device_id={AXIS: peer}, device_id_type=MESH
        )

    other = lax.rem(me + 1, n)

    def arrived(ref, sem):
        send(ref, ref, sem, sem, other).wait_recv()

    def left(ref, sem):
        send(ref, ref, sem, sem, other).wait_send()

    pairs = ((part, rs_data, dr_data), (stat, rs_stat, dr_stat))

    def rs_start(i):
        b, owner = i // n, lax.rem(i, n)

        @pl.when(owner != me)
        def _():
            for x, (src, dst, _) in enumerate(pairs):
                send(src.at[i], dst.at[b, me], rs_send.at[x], rs_recv.at[x, b], owner).start()

        @pl.when(owner == me)
        def _():
            for src, dst, _ in pairs:
                dst[b, me] = src[i]

    def ag_start(b):
        @pl.when(b * n + me < ringed)
        def _():
            for x, (_, ref, _) in enumerate(pairs):
                arrived(ref.at[b, pl.ds(0, n - 1)], rs_recv.at[x, b])
            s = b * n + me
            out[s] = together([rs_data[b, d] for d in range(n)], [rs_stat[b, d] for d in range(n)])
            for o in order:
                send(out.at[s], out.at[s], ag_send.at[b], ag_recv.at[b], lax.rem(me + o, n)).start()

    def dr_start(c):
        at, count = starts[c], CHUNKS[c]
        for o in order:
            for x, (src, _, dst) in enumerate(pairs):
                send(src.at[pl.ds(at, count)], dst.at[me, pl.ds(at - ringed, count)], dr_send.at[x, c], dr_recv.at[x, c], lax.rem(me + o, n)).start()
        for t in range(count):
            for src, _, dst in pairs:
                dst[me, at - ringed + t] = src[at + t]

    def dr_end(c):
        for x, (_, _, ref) in enumerate(pairs):
            arrived(ref.at[pl.ds(0, n - 1), pl.ds(starts[c] - ringed, CHUNKS[c])], dr_recv.at[x, c])
        for t in range(CHUNKS[c]):
            at = starts[c] - ringed + t
            out[starts[c] + t] = together([dr_data[d, at] for d in range(n)], [dr_stat[d, at] for d in range(n)])

    q_copy.wait()
    k_copy(0).wait()
    look(0, w0)

    def body(i, w_now, w_next):
        k_copy(i + 1).wait()
        v_copy(i).wait()
        look(i + 1, w_next)
        see(i, w_now)

    batches = -(-ringed // n)
    ag_at = [min((b + 1) * n, ringed) // 2 + 2 for b in range(batches)]

    def pair(p, send):
        for h, (w_now, w_next) in enumerate(((w0, w1), (w1, w0))):
            i = 2 * p + h

            @pl.when(i + SLOTS < seqs)
            def _():
                k_copy(i + SLOTS).start()

            v_start(i - 1 + SLOTS)
            body(i, w_now, w_next)
            if send:

                @pl.when(i - 1 < ringed)
                def _():
                    rs_start(i - 1)

    @pl.loop(0, EARLY)
    def _(p):
        pair(p, False)

    pl.semaphore_wait(barrier, n - 1)

    @pl.loop(0, 2 * EARLY - 1)
    def _(i):
        rs_start(i)

    @pl.loop(EARLY, seqs // 2 - 1)
    def _(p):
        pair(p, True)

        for b in range(batches):
            if ag_at[b] < seqs // 2 - 1:

                @pl.when(p == ag_at[b])
                def _():
                    ag_start(b)

    if ringed == seqs - 2:
        rs_start(ringed - 1)
    for c in range(len(CHUNKS)):
        if starts[c] + CHUNKS[c] <= seqs - 2:
            dr_start(c)
    body(seqs - 2, w0, w1)
    for c in range(len(CHUNKS)):
        if starts[c] + CHUNKS[c] == seqs - 1:
            dr_start(c)
    for b in range(batches):
        if ag_at[b] >= seqs // 2 - 1:
            ag_start(b)
    slot, step = (seqs - 1) % SLOTS, rows // TAIL
    o = jnp.zeros((heads, width), jnp.float32)
    for t in range(TAIL):
        v_piece(t).wait()
        o = o + jnp.dot(w1[:, t * step : (t + 1) * step], vbuf[slot, t * step : (t + 1) * step], preferred_element_type=jnp.float32)
    part[seqs - 1] = o.astype(jnp.bfloat16)
    dr_start(len(CHUNKS) - 1)

    for b in range(batches):
        here = min(n, ringed - b * n)

        @pl.when(me < here)
        def _():
            arrived(out.at[pl.ds(0, here - 1)], ag_recv.at[b])

        if here < n:

            @pl.when(me >= here)
            def _():
                arrived(out.at[pl.ds(0, here)], ag_recv.at[b])

    for c in range(len(CHUNKS)):
        dr_end(c)

    mine = -(-ringed // n)
    short = ringed % n or n

    @pl.when(me < short)
    def _():
        for x, (src, _, _) in enumerate(pairs):
            left(src.at[pl.ds(0, ringed - mine)], rs_send.at[x])

    if short < n:

        @pl.when(me >= short)
        def _():
            for x, (src, _, _) in enumerate(pairs):
                left(src.at[pl.ds(0, ringed - mine + 1)], rs_send.at[x])

    for b in range(batches):

        @pl.when(b * n + me < ringed)
        def _():
            left(out.at[pl.ds(0, n - 1)], ag_send.at[b])

    for c in range(len(CHUNKS)):
        for x, (_, _, ref) in enumerate(pairs):
            left(ref.at[pl.ds(0, n - 1), pl.ds(starts[c] - ringed, CHUNKS[c])], dr_send.at[x, c])


def solution(mesh):
    n = mesh.shape[AXIS]

    def step(q, k, v):
        seqs, tokens, heads, width = k.shape
        rows, direct = tokens * heads, sum(CHUNKS)
        ringed = seqs - direct
        batches, chunks = -(-ringed // n), len(CHUNKS)
        flat = lambda a: a.reshape(seqs, rows, width)
        dma = pltpu.SemaphoreType.DMA
        return pl.pallas_call(
            functools.partial(kernel, n, seqs, rows, heads, width, width**-0.5),
            out_shape=jax.ShapeDtypeStruct(q.shape, q.dtype),
            in_specs=[pl.BlockSpec(memory_space=pltpu.HBM)] * 3,
            out_specs=pl.BlockSpec(memory_space=pltpu.VMEM),
            scratch_shapes=[
                pltpu.VMEM(q.shape, q.dtype),
                pltpu.VMEM((SLOTS, rows, width), k.dtype),
                pltpu.VMEM((SLOTS, rows, width), v.dtype),
                pltpu.VMEM((heads, rows), jnp.bfloat16),
                pltpu.VMEM((heads, rows), jnp.bfloat16),
                pltpu.VMEM((seqs, heads, width), jnp.bfloat16),
                pltpu.VMEM((seqs, 1, LANES), jnp.float32),
                pltpu.VMEM((batches, n, heads, width), jnp.bfloat16),
                pltpu.VMEM((batches, n, 1, LANES), jnp.float32),
                pltpu.VMEM((n, direct, heads, width), jnp.bfloat16),
                pltpu.VMEM((n, direct, 1, LANES), jnp.float32),
                dma(()),
                dma((SLOTS,)),
                dma((SLOTS,)),
                dma((TAIL,)),
                dma((2,)),
                dma((2, batches)),
                dma((batches,)),
                dma((batches,)),
                dma((2, chunks)),
                dma((2, chunks)),
            ],
            compiler_params=pltpu.CompilerParams(
                collective_id=COLLECTIVE, has_side_effects=True, vmem_limit_bytes=40 * 1024 * 1024
            ),
            cost_estimate=pl.CostEstimate(flops=4 * seqs * rows * width, bytes_accessed=2 * k.size * 2, transcendentals=0),
            name="attend",
        )(q, flat(k), flat(v))

    return jax.shard_map(
        step,
        mesh=mesh,
        in_specs=(P("dp", None, None), P("dp", AXIS, None, None), P("dp", AXIS, None, None)),
        out_specs=P("dp", None, None),
        check_vma=False,
    )
```

```python
import functools
import math

import jax
import jax.numpy as jnp
from jax import lax
from jax.experimental import pallas as pl
from jax.experimental.pallas import tpu as pltpu
from jax.sharding import PartitionSpec as P

FLIGHT = 3
SLOTS = FLIGHT + 1
AHEAD = 1
LAST = 1
EARLY = 10
TAIL = 2
LATER = 4
CHUNKS = (3, 2)
LANES = 128
AXIS = "sp"
MESH = pl.DeviceIdType.MESH
COLLECTIVE = 0


def offsets(n):
    side = math.isqrt(n)
    near = lambda a: min(a, side - a)
    return sorted(range(1, n), key=lambda o: -(near(o // side % side) + near(o % side)))


def kernel(
    n, seqs, rows, heads, width, scale,
    q_hbm, k_hbm, v_hbm, out,
    qbuf, kbuf, vbuf, wbuf, part, stat,
    rs_data, rs_stat, dr_data, dr_stat,
    qsem, ksem, vsem, tsem,
    rs_send, rs_recv, ag_send, ag_recv, dr_send, dr_recv, st_sem,
):
    me = lax.axis_index(AXIS)
    direct = sum(CHUNKS)
    ringed = seqs - direct
    starts = [ringed + sum(CHUNKS[:c]) for c in range(len(CHUNKS))]
    order = offsets(n)

    def k_copy(i):
        slot = lax.rem(i, SLOTS)
        return pltpu.make_async_copy(k_hbm.at[i], kbuf.at[slot], ksem.at[slot])

    def v_copy(i):
        slot = lax.rem(i, SLOTS)
        return pltpu.make_async_copy(v_hbm.at[i], vbuf.at[slot], vsem.at[slot])

    def v_piece(t):
        at, slot = pl.ds(t * (rows // TAIL), rows // TAIL), (seqs - 1) % SLOTS
        return pltpu.make_async_copy(v_hbm.at[seqs - 1, at], vbuf.at[slot, at], tsem.at[t])

    def k_piece(t):
        at = pl.ds(t * (rows // TAIL), rows // TAIL)
        return pltpu.make_async_copy(k_hbm.at[0, at], kbuf.at[0, at], tsem.at[t])

    def k_start(i):
        @pl.when(i < seqs)
        def _():
            k_copy(i).start()

    def v_start(i):
        @pl.when(i < seqs - 1)
        def _():
            v_copy(i).start()

        @pl.when(i == seqs - 1)
        def _():
            for t in range(TAIL):
                v_piece(t).start()

    q_copy = pltpu.make_async_copy(q_hbm, qbuf, qsem)
    q_copy.start()
    for t in range(TAIL):
        k_piece(t).start()
    for i in range(1, FLIGHT):
        k_start(i)
    for i in range(FLIGHT):
        v_start(i)

    barrier = pltpu.get_barrier_semaphore()
    for o in order:
        pl.semaphore_signal(barrier, inc=1, device_id={AXIS: lax.rem(me + o, n)}, device_id_type=MESH)

    lane = lax.broadcasted_iota(jnp.int32, (heads, LANES), 1)
    sub = lax.broadcasted_iota(jnp.int32, (heads, LANES), 0)
    own = lane % heads == sub
    diag = lane == sub
    diag2 = lane == sub + heads

    def look(i):
        i = jnp.int32(i)
        slot, w = lax.rem(i, SLOTS), lax.rem(i, AHEAD + 1)
        s = lax.dot_general(qbuf[i], kbuf[slot], (((1,), (1,)), ((), ())), preferred_element_type=jnp.float32)
        cols = [jnp.where(own, s[:, c : c + LANES], -jnp.inf) for c in range(0, rows, LANES)]
        high = jnp.max(functools.reduce(jnp.maximum, cols), 1, keepdims=True)
        total = jnp.zeros((heads, LANES), jnp.float32)
        for c, col in enumerate(cols):
            e = jnp.exp((col - high) * scale)
            total = total + e
            wbuf[w, :, c * LANES : (c + 1) * LANES] = e.astype(jnp.bfloat16)
        total = jnp.sum(total, 1, keepdims=True)
        row = jnp.where(diag, high * scale, 0.0) + jnp.where(diag2, total, 0.0)
        stat[i] = jnp.sum(row, 0, keepdims=True)

    def see(i):
        slot, w = lax.rem(i, SLOTS), lax.rem(i, AHEAD + 1)
        o = jnp.dot(wbuf[w], vbuf[slot], preferred_element_type=jnp.float32)
        part[i] = o.astype(jnp.bfloat16)

    def shares(stats):
        high = functools.reduce(jnp.maximum, stats)
        f = [jnp.exp(s - high) for s in stats]
        total = functools.reduce(jnp.add, [a * pltpu.roll(s, LANES - heads, 1) for a, s in zip(f, stats)])
        column = lambda r: jnp.sum(jnp.where(diag, jnp.broadcast_to(r, (heads, LANES)), 0.0), 1, keepdims=True)
        return [column(a) for a in f], column(total)

    def together(data, counts):
        f, total = counts
        seen = functools.reduce(jnp.add, [a * d.astype(jnp.float32) for a, d in zip(f, data)])
        return (seen / total).astype(jnp.bfloat16)

    def send(src, dst, send_sem, recv_sem, peer):
        return pltpu.make_async_remote_copy(
            src_ref=src, dst_ref=dst, send_sem=send_sem, recv_sem=recv_sem, device_id={AXIS: peer}, device_id_type=MESH
        )

    other = lax.rem(me + 1, n)

    def arrived(ref, sem):
        send(ref, ref, sem, sem, other).wait_recv()

    def left(ref, sem):
        send(ref, ref, sem, sem, other).wait_send()

    pairs = ((part, rs_data), (stat, rs_stat))

    def rs_start(i):
        b, owner = i // n, lax.rem(i, n)

        @pl.when(owner != me)
        def _():
            for x, (src, dst) in enumerate(pairs):
                send(src.at[i], dst.at[b, me], rs_send.at[x], rs_recv.at[x, b], owner).start()

        @pl.when(owner == me)
        def _():
            for src, dst in pairs:
                dst[b, me] = src[i]

    def ag_start(b):
        @pl.when(b * n + me < ringed)
        def _():
            for x, (_, ref) in enumerate(pairs):
                arrived(ref.at[b, pl.ds(0, n - 1)], rs_recv.at[x, b])
            s = b * n + me
            out[s] = together([rs_data[b, d] for d in range(n)], shares([rs_stat[b, d] for d in range(n)]))
            for o in order:
                send(out.at[s], out.at[s], ag_send.at[b], ag_recv.at[b], lax.rem(me + o, n)).start()

    tops = pl.ds(ringed, direct)

    def tops_start():
        for t in range(direct):
            dr_stat[me, t] = stat[ringed + t]
        for o in order:
            send(stat.at[tops], dr_stat.at[me], st_sem.at[0], st_sem.at[1], lax.rem(me + o, n)).start()

    def dr_start(c):
        at, count = starts[c], CHUNKS[c]
        for t in range(count):
            dr_data[me, at - ringed + t] = part[at + t]
        for o in order:
            send(part.at[pl.ds(at, count)], dr_data.at[me, pl.ds(at - ringed, count)], dr_send.at[c], dr_recv.at[c], lax.rem(me + o, n)).start()

    def dr_end(c):
        at, count = starts[c] - ringed, CHUNKS[c]
        counts = [shares([dr_stat[d, at + t] for d in range(n)]) for t in range(count)]
        arrived(dr_data.at[pl.ds(0, n - 1), pl.ds(at, count)], dr_recv.at[c])
        for t in range(count):
            out[starts[c] + t] = together([dr_data[d, at + t] for d in range(n)], counts[t])

    batches = -(-ringed // n)
    ag_at = [min((b + 1) * n, ringed) - 1 + LATER for b in range(batches)]
    steady = seqs - AHEAD - LAST

    q_copy.wait()
    for t in range(TAIL):
        k_piece(t).wait()
    k_start(FLIGHT)
    look(0)

    @pl.loop(1, AHEAD)
    def _(i):
        k_copy(i).wait()
        k_start(i + FLIGHT)
        look(i)

    def body(i):
        k_copy(i + AHEAD).wait()
        k_start(i + AHEAD + FLIGHT)
        v_copy(i).wait()
        v_start(i + FLIGHT)
        see(i)
        look(i + AHEAD)

    @pl.loop(0, EARLY)
    def _(i):
        body(i)

    pl.semaphore_wait(barrier, n - 1)

    @pl.loop(0, EARLY - 1)
    def _(i):
        rs_start(i)

    @pl.loop(EARLY, steady)
    def _(i):
        body(i)

        @pl.when(i - 1 < ringed)
        def _():
            rs_start(i - 1)

        for b in range(batches):
            if ag_at[b] < steady:

                @pl.when(i == ag_at[b])
                def _():
                    ag_start(b)

        for c in range(len(CHUNKS)):
            if starts[c] + CHUNKS[c] - 1 < steady:

                @pl.when(i == starts[c] + CHUNKS[c] - 1)
                def _():
                    dr_start(c)

    def after(i):
        if i - 1 < ringed:
            rs_start(i - 1)
        for c in range(len(CHUNKS)):
            if starts[c] + CHUNKS[c] - 1 == i:
                dr_start(c)
        for b in range(batches):
            if ag_at[b] == i:
                ag_start(b)

    for i in range(steady, seqs - 1):
        if i + AHEAD < seqs:
            k_copy(i + AHEAD).wait()
            k_start(i + AHEAD + FLIGHT)
            look(i + AHEAD)
        if i + AHEAD == seqs - 1:
            tops_start()
        v_copy(i).wait()
        v_start(i + FLIGHT)
        see(i)
        after(i)

    slot, step = (seqs - 1) % SLOTS, rows // TAIL
    w = (seqs - 1) % (AHEAD + 1)
    o = jnp.zeros((heads, width), jnp.float32)
    for t in range(TAIL):
        v_piece(t).wait()
        at = slice(t * step, (t + 1) * step)
        o = o + jnp.dot(wbuf[w, :, at], vbuf[slot, at], preferred_element_type=jnp.float32)
    part[seqs - 1] = o.astype(jnp.bfloat16)
    after(seqs - 1)

    for b in range(batches):
        here = min(n, ringed - b * n)

        @pl.when(me < here)
        def _():
            arrived(out.at[pl.ds(0, here - 1)], ag_recv.at[b])

        if here < n:

            @pl.when(me >= here)
            def _():
                arrived(out.at[pl.ds(0, here)], ag_recv.at[b])

    arrived(dr_stat.at[pl.ds(0, n - 1)], st_sem.at[1])
    for c in range(len(CHUNKS)):
        dr_end(c)

    mine = -(-ringed // n)
    short = ringed % n or n

    @pl.when(me < short)
    def _():
        for x, (src, _) in enumerate(pairs):
            left(src.at[pl.ds(0, ringed - mine)], rs_send.at[x])

    if short < n:

        @pl.when(me >= short)
        def _():
            for x, (src, _) in enumerate(pairs):
                left(src.at[pl.ds(0, ringed - mine + 1)], rs_send.at[x])

    for b in range(batches):

        @pl.when(b * n + me < ringed)
        def _():
            left(out.at[pl.ds(0, n - 1)], ag_send.at[b])

    for c in range(len(CHUNKS)):
        left(dr_data.at[pl.ds(0, n - 1), pl.ds(starts[c] - ringed, CHUNKS[c])], dr_send.at[c])
    left(dr_stat.at[pl.ds(0, n - 1)], st_sem.at[0])


def solution(mesh):
    n = mesh.shape[AXIS]

    def step(q, k, v):
        seqs, tokens, heads, width = k.shape
        rows, direct = tokens * heads, sum(CHUNKS)
        ringed = seqs - direct
        batches, chunks = -(-ringed // n), len(CHUNKS)
        flat = lambda a: a.reshape(seqs, rows, width)
        dma = pltpu.SemaphoreType.DMA
        return pl.pallas_call(
            functools.partial(kernel, n, seqs, rows, heads, width, width**-0.5),
            out_shape=jax.ShapeDtypeStruct(q.shape, q.dtype),
            in_specs=[pl.BlockSpec(memory_space=pltpu.HBM)] * 3,
            out_specs=pl.BlockSpec(memory_space=pltpu.VMEM),
            scratch_shapes=[
                pltpu.VMEM(q.shape, q.dtype),
                pltpu.VMEM((SLOTS, rows, width), k.dtype),
                pltpu.VMEM((SLOTS, rows, width), v.dtype),
                pltpu.VMEM((AHEAD + 1, heads, rows), jnp.bfloat16),
                pltpu.VMEM((seqs, heads, width), jnp.bfloat16),
                pltpu.VMEM((seqs, 1, LANES), jnp.float32),
                pltpu.VMEM((batches, n, heads, width), jnp.bfloat16),
                pltpu.VMEM((batches, n, 1, LANES), jnp.float32),
                pltpu.VMEM((n, direct, heads, width), jnp.bfloat16),
                pltpu.VMEM((n, direct, 1, LANES), jnp.float32),
                dma(()),
                dma((SLOTS,)),
                dma((SLOTS,)),
                dma((TAIL,)),
                dma((2,)),
                dma((2, batches)),
                dma((batches,)),
                dma((batches,)),
                dma((chunks,)),
                dma((chunks,)),
                dma((2,)),
            ],
            compiler_params=pltpu.CompilerParams(
                collective_id=COLLECTIVE, has_side_effects=True, vmem_limit_bytes=40 * 1024 * 1024
            ),
            cost_estimate=pl.CostEstimate(flops=4 * seqs * rows * width, bytes_accessed=2 * k.size * 2, transcendentals=0),
            name="attend",
        )(pltpu.with_memory_space_constraint(q, pltpu.HBM), flat(k), flat(v))

    return jax.shard_map(
        step,
        mesh=mesh,
        in_specs=(P("dp", None, None), P("dp", AXIS, None, None), P("dp", AXIS, None, None)),
        out_specs=P("dp", None, None),
        check_vma=False,
    )
```

```python
import functools
import math

import jax
import jax.numpy as jnp
from jax import lax
from jax.experimental import pallas as pl
from jax.experimental.pallas import tpu as pltpu
from jax.sharding import PartitionSpec as P

FLIGHT = 3
SLOTS = FLIGHT + 1
AHEAD = 1
LAST = 1
EARLY = 10
TAIL = 1
LATER = 4
CHUNKS = (3, 2)
LANES = 128
AXIS = "sp"
MESH = pl.DeviceIdType.MESH
COLLECTIVE = 0


def offsets(n):
    side = math.isqrt(n)
    near = lambda a: min(a, side - a)
    steps = [(a, b) for a in range(side) for b in range(side) if a or b]
    return sorted(steps, key=lambda s: -(near(s[0]) + near(s[1])))


def kernel(
    n, seqs, rows, heads, width, scale,
    q_hbm, k_hbm, v_hbm, out,
    qbuf, kbuf, vbuf, wbuf, part, stat,
    rs_data, rs_stat, dr_data, dr_stat,
    qsem, ksem, vsem, tsem,
    rs_send, rs_recv, ag_send, ag_recv, dr_send, dr_recv, st_sem,
):
    me = lax.axis_index(AXIS)
    direct = sum(CHUNKS)
    ringed = seqs - direct
    starts = [ringed + sum(CHUNKS[:c]) for c in range(len(CHUNKS))]
    order, side = offsets(n), math.isqrt(n)
    peer = lambda o: lax.rem(me // side + o[0], side) * side + lax.rem(me + o[1], side)

    def k_copy(i):
        slot = lax.rem(i, SLOTS)
        return pltpu.make_async_copy(k_hbm.at[i], kbuf.at[slot], ksem.at[slot])

    def v_copy(i):
        slot = lax.rem(i, SLOTS)
        return pltpu.make_async_copy(v_hbm.at[i], vbuf.at[slot], vsem.at[slot])

    def v_piece(t):
        at, slot = pl.ds(t * (rows // TAIL), rows // TAIL), (seqs - 1) % SLOTS
        return pltpu.make_async_copy(v_hbm.at[seqs - 1, at], vbuf.at[slot, at], tsem.at[t])

    def k_piece(t):
        at = pl.ds(t * (rows // TAIL), rows // TAIL)
        return pltpu.make_async_copy(k_hbm.at[0, at], kbuf.at[0, at], tsem.at[t])

    def k_start(i):
        @pl.when(i < seqs)
        def _():
            k_copy(i).start()

    def v_start(i):
        @pl.when(i < seqs - 1)
        def _():
            v_copy(i).start()

        @pl.when(i == seqs - 1)
        def _():
            for t in range(TAIL):
                v_piece(t).start()

    q_copy = pltpu.make_async_copy(q_hbm, qbuf, qsem)
    q_copy.start()
    for t in range(TAIL):
        k_piece(t).start()
    for i in range(1, FLIGHT):
        k_start(i)
    for i in range(FLIGHT - 1):
        v_start(i)

    barrier = pltpu.get_barrier_semaphore()
    for o in order:
        pl.semaphore_signal(barrier, inc=1, device_id={AXIS: peer(o)}, device_id_type=MESH)

    lane = lax.broadcasted_iota(jnp.int32, (heads, LANES), 1)
    sub = lax.broadcasted_iota(jnp.int32, (heads, LANES), 0)
    own = lane % heads == sub
    diag = lane == sub
    diag2 = lane == sub + heads

    def look(i):
        i = jnp.int32(i)
        slot, w = lax.rem(i, SLOTS), lax.rem(i, AHEAD + 1)
        s = lax.dot_general(qbuf[i], kbuf[slot], (((1,), (1,)), ((), ())), preferred_element_type=jnp.float32)
        cols = [jnp.where(own, s[:, c : c + LANES], -jnp.inf) for c in range(0, rows, LANES)]
        high = jnp.max(functools.reduce(jnp.maximum, cols), 1, keepdims=True)
        total = jnp.zeros((heads, LANES), jnp.float32)
        for c, col in enumerate(cols):
            e = jnp.exp((col - high) * scale)
            total = total + e
            wbuf[w, :, c * LANES : (c + 1) * LANES] = e.astype(jnp.bfloat16)
        total = jnp.sum(total, 1, keepdims=True)
        row = jnp.where(diag, high * scale, 0.0) + jnp.where(diag2, total, 0.0)
        stat[i] = jnp.sum(row, 0, keepdims=True)

    def see(i):
        slot, w = lax.rem(i, SLOTS), lax.rem(i, AHEAD + 1)
        o = jnp.dot(wbuf[w], vbuf[slot], preferred_element_type=jnp.float32)
        part[i] = o.astype(jnp.bfloat16)

    def shares(stats):
        high = functools.reduce(jnp.maximum, stats)
        f = [jnp.exp(s - high) for s in stats]
        total = functools.reduce(jnp.add, [a * pltpu.roll(s, LANES - heads, 1) for a, s in zip(f, stats)])
        column = lambda r: jnp.sum(jnp.where(diag, jnp.broadcast_to(r, (heads, LANES)), 0.0), 1, keepdims=True)
        return [column(a) for a in f], column(total)

    def together(data, counts):
        f, total = counts
        seen = functools.reduce(jnp.add, [a * d.astype(jnp.float32) for a, d in zip(f, data)])
        return (seen / total).astype(jnp.bfloat16)

    def send(src, dst, send_sem, recv_sem, peer):
        return pltpu.make_async_remote_copy(
            src_ref=src, dst_ref=dst, send_sem=send_sem, recv_sem=recv_sem, device_id={AXIS: peer}, device_id_type=MESH
        )

    other = lax.rem(me + 1, n)

    def arrived(ref, sem):
        send(ref, ref, sem, sem, other).wait_recv()

    def left(ref, sem):
        send(ref, ref, sem, sem, other).wait_send()

    pairs = ((part, rs_data), (stat, rs_stat))

    def rs_start(i):
        b, owner = i // n, lax.rem(i, n)

        @pl.when(owner != me)
        def _():
            for x, (src, dst) in enumerate(pairs):
                send(src.at[i], dst.at[b, me], rs_send.at[x], rs_recv.at[x, b], owner).start()

        @pl.when(owner == me)
        def _():
            for src, dst in pairs:
                dst[b, me] = src[i]

    def ag_start(b):
        @pl.when(b * n + me < ringed)
        def _():
            for x, (_, ref) in enumerate(pairs):
                arrived(ref.at[b, pl.ds(0, n - 1)], rs_recv.at[x, b])
            s = b * n + me
            out[s] = together([rs_data[b, d] for d in range(n)], shares([rs_stat[b, d] for d in range(n)]))
            for o in order:
                send(out.at[s], out.at[s], ag_send.at[b], ag_recv.at[b], peer(o)).start()

    tops = pl.ds(ringed, direct)

    def tops_start():
        for t in range(direct):
            dr_stat[me, t] = stat[ringed + t]
        for o in order:
            send(stat.at[tops], dr_stat.at[me], st_sem.at[0], st_sem.at[1], peer(o)).start()

    def dr_start(c):
        at, count = starts[c], CHUNKS[c]
        for t in range(count):
            dr_data[me, at - ringed + t] = part[at + t]
        for o in order:
            send(part.at[pl.ds(at, count)], dr_data.at[me, pl.ds(at - ringed, count)], dr_send.at[c], dr_recv.at[c], peer(o)).start()

    def dr_end(c):
        at, count = starts[c] - ringed, CHUNKS[c]
        counts = [shares([dr_stat[d, at + t] for d in range(n)]) for t in range(count)]
        arrived(dr_data.at[pl.ds(0, n - 1), pl.ds(at, count)], dr_recv.at[c])
        for t in range(count):
            out[starts[c] + t] = together([dr_data[d, at + t] for d in range(n)], counts[t])

    batches = -(-ringed // n)
    ag_at = [min((b + 1) * n, ringed) - 1 + LATER for b in range(batches)]
    steady = seqs - AHEAD - LAST

    q_copy.wait()
    for t in range(TAIL):
        k_piece(t).wait()
    k_start(FLIGHT)
    v_start(FLIGHT - 1)
    look(0)

    @pl.loop(1, AHEAD)
    def _(i):
        k_copy(i).wait()
        k_start(i + FLIGHT)
        look(i)

    def body(i):
        k_copy(i + AHEAD).wait()
        k_start(i + AHEAD + FLIGHT)
        v_copy(i).wait()
        v_start(i + FLIGHT)
        see(i)
        look(i + AHEAD)

    @pl.loop(0, EARLY)
    def _(i):
        body(i)

    pl.semaphore_wait(barrier, n - 1)

    @pl.loop(0, EARLY - 1)
    def _(i):
        rs_start(i)

    @pl.loop(EARLY, steady)
    def _(i):
        body(i)

        @pl.when(i - 1 < ringed)
        def _():
            rs_start(i - 1)

        for b in range(batches):
            if ag_at[b] < steady:

                @pl.when(i == ag_at[b])
                def _():
                    ag_start(b)

        for c in range(len(CHUNKS)):
            if starts[c] + CHUNKS[c] - 1 < steady:

                @pl.when(i == starts[c] + CHUNKS[c] - 1)
                def _():
                    dr_start(c)

    def after(i):
        if i - 1 < ringed:
            rs_start(i - 1)
        for c in range(len(CHUNKS)):
            if starts[c] + CHUNKS[c] - 1 == i:
                dr_start(c)
        for b in range(batches):
            if ag_at[b] == i:
                ag_start(b)

    for i in range(steady, seqs - 1):
        if i + AHEAD < seqs:
            k_copy(i + AHEAD).wait()
            k_start(i + AHEAD + FLIGHT)
            look(i + AHEAD)
        if i + AHEAD == seqs - 1:
            tops_start()
        v_copy(i).wait()
        v_start(i + FLIGHT)
        see(i)
        after(i)

    slot, step = (seqs - 1) % SLOTS, rows // TAIL
    w = (seqs - 1) % (AHEAD + 1)
    o = jnp.zeros((heads, width), jnp.float32)
    for t in range(TAIL):
        v_piece(t).wait()
        at = slice(t * step, (t + 1) * step)
        o = o + jnp.dot(wbuf[w, :, at], vbuf[slot, at], preferred_element_type=jnp.float32)
    part[seqs - 1] = o.astype(jnp.bfloat16)
    after(seqs - 1)

    for b in range(batches):
        here = min(n, ringed - b * n)

        @pl.when(me < here)
        def _():
            arrived(out.at[pl.ds(0, here - 1)], ag_recv.at[b])

        if here < n:

            @pl.when(me >= here)
            def _():
                arrived(out.at[pl.ds(0, here)], ag_recv.at[b])

    arrived(dr_stat.at[pl.ds(0, n - 1)], st_sem.at[1])
    for c in range(len(CHUNKS)):
        dr_end(c)

    mine = -(-ringed // n)
    short = ringed % n or n

    @pl.when(me < short)
    def _():
        for x, (src, _) in enumerate(pairs):
            left(src.at[pl.ds(0, ringed - mine)], rs_send.at[x])

    if short < n:

        @pl.when(me >= short)
        def _():
            for x, (src, _) in enumerate(pairs):
                left(src.at[pl.ds(0, ringed - mine + 1)], rs_send.at[x])

    for b in range(batches):

        @pl.when(b * n + me < ringed)
        def _():
            left(out.at[pl.ds(0, n - 1)], ag_send.at[b])

    for c in range(len(CHUNKS)):
        left(dr_data.at[pl.ds(0, n - 1), pl.ds(starts[c] - ringed, CHUNKS[c])], dr_send.at[c])
    left(dr_stat.at[pl.ds(0, n - 1)], st_sem.at[0])


def solution(mesh):
    n = mesh.shape[AXIS]

    def step(q, k, v):
        seqs, tokens, heads, width = k.shape
        rows, direct = tokens * heads, sum(CHUNKS)
        ringed = seqs - direct
        batches, chunks = -(-ringed // n), len(CHUNKS)
        flat = lambda a: a.reshape(seqs, rows, width)
        dma = pltpu.SemaphoreType.DMA
        return pl.pallas_call(
            functools.partial(kernel, n, seqs, rows, heads, width, width**-0.5),
            out_shape=jax.ShapeDtypeStruct(q.shape, q.dtype),
            in_specs=[pl.BlockSpec(memory_space=pltpu.HBM)] * 3,
            out_specs=pl.BlockSpec(memory_space=pltpu.VMEM),
            scratch_shapes=[
                pltpu.VMEM(q.shape, q.dtype),
                pltpu.VMEM((SLOTS, rows, width), k.dtype),
                pltpu.VMEM((SLOTS, rows, width), v.dtype),
                pltpu.VMEM((AHEAD + 1, heads, rows), jnp.bfloat16),
                pltpu.VMEM((seqs, heads, width), jnp.bfloat16),
                pltpu.VMEM((seqs, 1, LANES), jnp.float32),
                pltpu.VMEM((batches, n, heads, width), jnp.bfloat16),
                pltpu.VMEM((batches, n, 1, LANES), jnp.float32),
                pltpu.VMEM((n, direct, heads, width), jnp.bfloat16),
                pltpu.VMEM((n, direct, 1, LANES), jnp.float32),
                dma(()),
                dma((SLOTS,)),
                dma((SLOTS,)),
                dma((TAIL,)),
                dma((2,)),
                dma((2, batches)),
                dma((batches,)),
                dma((batches,)),
                dma((chunks,)),
                dma((chunks,)),
                dma((2,)),
            ],
            compiler_params=pltpu.CompilerParams(
                collective_id=COLLECTIVE, has_side_effects=True, vmem_limit_bytes=40 * 1024 * 1024
            ),
            cost_estimate=pl.CostEstimate(flops=4 * seqs * rows * width, bytes_accessed=2 * k.size * 2, transcendentals=0),
            name="attend",
        )(pltpu.with_memory_space_constraint(q, pltpu.HBM), flat(k), flat(v))

    return jax.shard_map(
        step,
        mesh=mesh,
        in_specs=(P("dp", None, None), P("dp", AXIS, None, None), P("dp", AXIS, None, None)),
        out_specs=P("dp", None, None),
        check_vma=False,
    )
```
